256 devices in a mesh: shard: 64 (over z, x, core), width: 4 (over y).
Axes of the slice: x: 4, y: 4, z: 8, core: 2. Of those that a mesh axis runs over, the one named last changes fastest.
Arguments:
- w_query: float32 [4096, 4096], P('shard', 'width'), may hold values from -0.25 to 0.25
- first_query: float32 [4096, 4096], P('shard', 'width'), may hold values from -0.09375 to 0.09375
- second_query: float32 [4096, 4096], P('shard', 'width'), may hold values from -0.09375 to 0.09375
- w_key: float32 [4096, 1024], P('shard', 'width'), may hold values from -0.25 to 0.25
- first_key: float32 [4096, 1024], P('shard', 'width'), may hold values from -0.09375 to 0.09375
- second_key: float32 [4096, 1024], P('shard', 'width'), may hold values from -0.09375 to 0.09375
- w_value: float32 [4096, 1024], P('shard', 'width'), may hold values from -0.25 to 0.25
- first_value: float32 [4096, 1024], P('shard', 'width'), may hold values from -0.09375 to 0.09375
- second_value: float32 [4096, 1024], P('shard', 'width'), may hold values from -0.09375 to 0.09375
- norm_train: float32 [4096], P(('shard', 'width')), may hold values from 0.25 to 1.75
- norm_step: float32 [4096], P(('shard', 'width')), may hold values from -0.3 to 0.3
Outputs:
- serving_query: bfloat16 [4096, 4096], P(None, 'width')
- serving_key: bfloat16 [4096, 1024], P(None, 'width')
- serving_value: bfloat16 [4096, 1024], P(None, 'width')
- column_query: float32 [4096], P('width')
- column_key: float32 [1024], P('width')
- column_value: float32 [1024], P('width')
- serve_norm: bfloat16 [4096], replicated
- whole_query: float32 [4096, 4096], P('shard', 'width')
- whole_key: float32 [4096, 1024], P('shard', 'width')
- whole_value: float32 [4096, 1024], P('shard', 'width')
The draws below stay inside these ranges and needn't reach their ends.
All inputs are finite; a program needn't handle non-finite values. Where the reference program divides by a largest or mean magnitude, that divisor is 1e-20 or more.
Results may differ from the reference program's by a relative error of at most 0.0004.
Values may be sent and summed in bfloat16 or wider, within the bound.
No kernel may reach another device: no remote copies, remote signals or barrier semaphores. Data moves between devices by JAX's collectives and lax.ppermute only.
A program may use at most 128 MiB of HBM per device.

```python
import jax
import jax.numpy as jnp

D_MODEL = 4096
Q_DIM = 4096
KV_DIM = 1024


def raised(entries, stream_key, source, target, parts, factor):
    owner, partner = [(jnp.arange(entries.shape[dim]) // (entries.shape[dim] // parts)).reshape([-1 if axis == dim else 1 for axis in range(entries.ndim)]) for dim in (source, target)]
    chosen = jax.random.permutation(stream_key, parts)[partner]
    strong = (owner == chosen) | (owner == (partner + parts // 2) % parts)
    return jnp.where(strong, factor * entries, entries)


def block_levels(own_key, shape, pieces, least, high):
    loudness = 1.0
    for dim, parts in pieces:
        steps = jax.random.uniform(jax.random.fold_in(jax.random.fold_in(own_key, 6), dim), (parts,), jnp.float32, least / len(pieces), high / len(pieces))
        loudness = loudness * jnp.repeat(jnp.exp(steps), shape[dim] // parts).reshape((-1,) + (1,) * (len(shape) - 1 - dim))
    return loudness


def scatter_about(key, extent, spread, most, split=(), held_as=jnp.bfloat16):
    array = spread * jax.random.normal(key, extent, jnp.float32)
    if split:
        array = array * block_levels(key, extent, split, -0.22, 0.18)
    return jnp.clip(array, -most, most).astype(held_as)


def gaussian_with(stream_key, dims, deviation, reach, split, heavy, held_as=jnp.bfloat16):
    values = deviation * jax.random.normal(stream_key, dims, jnp.float32)
    if split:
        values = values * block_levels(stream_key, dims, split, -0.22, 0.18)
    return jnp.clip(raised(values, jax.random.fold_in(stream_key, 3), *heavy), -reach, reach).astype(held_as)


def setup_inputs(seed: int = 0) -> dict:
    seeds = jax.random.split(jax.random.key(seed), 12)
    return {
        "w_query": gaussian_with(seeds[0], (D_MODEL, Q_DIM), D_MODEL ** -0.5, 0.25, ((0, 64), (1, 4)), (0, 1, 64, 4.0), jnp.float32),
        "first_query": scatter_about(seeds[1], (D_MODEL, Q_DIM), D_MODEL ** -0.5, 0.09375, ((0, 64), (1, 4)), jnp.float32),
        "second_query": scatter_about(seeds[2], (D_MODEL, Q_DIM), D_MODEL ** -0.5, 0.09375, ((0, 64), (1, 4)), jnp.float32),
        "w_key": gaussian_with(seeds[3], (D_MODEL, KV_DIM), D_MODEL ** -0.5, 0.25, ((0, 64), (1, 4)), (0, 1, 64, 4.0), jnp.float32),
        "first_key": scatter_about(seeds[4], (D_MODEL, KV_DIM), D_MODEL ** -0.5, 0.09375, ((0, 64), (1, 4)), jnp.float32),
        "second_key": scatter_about(seeds[5], (D_MODEL, KV_DIM), D_MODEL ** -0.5, 0.09375, ((0, 64), (1, 4)), jnp.float32),
        "w_value": gaussian_with(seeds[6], (D_MODEL, KV_DIM), D_MODEL ** -0.5, 0.25, ((0, 64), (1, 4)), (0, 1, 64, 4.0), jnp.float32),
        "first_value": scatter_about(seeds[7], (D_MODEL, KV_DIM), D_MODEL ** -0.5, 0.09375, ((0, 64), (1, 4)), jnp.float32),
        "second_value": scatter_about(seeds[8], (D_MODEL, KV_DIM), D_MODEL ** -0.5, 0.09375, ((0, 64), (1, 4)), jnp.float32),
        "norm_train": jnp.clip(1.0 + 0.15 * jax.random.normal(seeds[9], (D_MODEL,), jnp.float32), 0.25, 1.75),
        "norm_step": jnp.clip(jax.random.uniform(seeds[10], (D_MODEL,), jnp.float32, -0.3, 0.3) * block_levels(seeds[10], (D_MODEL,), ((0, 256),), -0.4, 0.0), -0.3, 0.3),
    }


learn_rate = 0.2
hold_rate = 0.8


def reference(w_query, first_query, second_query, w_key, first_key, second_key, w_value, first_value, second_value, norm_train, norm_step):
    hold_query = hold_rate * first_query + second_query
    whole_query = w_query - learn_rate * hold_query
    hold_key = hold_rate * first_key + second_key
    whole_key = w_key - learn_rate * hold_key
    hold_value = hold_rate * first_value + second_value
    whole_value = w_value - learn_rate * hold_value
    column_query = jnp.sum(jnp.abs(whole_query), axis=0) / D_MODEL
    serving_query = (whole_query / column_query).astype(jnp.bfloat16)
    column_key = jnp.sum(jnp.abs(whole_key), axis=0) / D_MODEL
    serving_key = (whole_key / column_key).astype(jnp.bfloat16)
    column_value = jnp.sum(jnp.abs(whole_value), axis=0) / D_MODEL
    serving_value = (whole_value / column_value).astype(jnp.bfloat16)
    serve_norm = (norm_train + norm_step).astype(jnp.bfloat16)
    return serving_query, serving_key, serving_value, column_query, column_key, column_value, serve_norm, whole_query, whole_key, whole_value
```

```python
import functools

import jax
import jax.numpy as jnp
from jax import lax
from jax.experimental import pallas as pl
from jax.experimental.pallas import tpu as pltpu
from jax.sharding import Mesh
from jax.sharding import PartitionSpec as P

D_MODEL = 4096
ZS, XS, CS, YS = 8, 4, 2, 4
SHARD = ("shard_0", "shard_1", "shard_2")
SHARD_WIDTH = ("shard_0", "shard_1", "shard_2", "width")
ROWS = 64
EXTRA = 128

learn_rate = 0.2
hold_rate = 0.8


def exchange(array, dim, phase):
    size = {"z": ZS, "x": XS}[dim]
    pairs = []
    for z in range(ZS):
        for x in range(XS):
            for c in range(CS):
                at = z if dim == "z" else x
                sign = 1 if (at + c) % 2 == 0 else -1
                to = (at + (sign if phase == 0 else -sign)) % size
                tz, tx = (to, x) if dim == "z" else (z, to)
                pairs.append(((z * XS + x) * CS + c, (tz * XS + tx) * CS + c))
    return lax.ppermute(array, SHARD, pairs)


def swap_cores(array):
    return lax.ppermute(array, "shard_2", [(0, 1), (1, 0)])


def assemble(kinds, offsets, *refs):
    n = len(kinds)
    pieces, (query, key, value), sem = refs[:n], refs[n : n + 3], refs[n + 3]
    z, x, c = (lax.axis_index(name) for name in SHARD)
    copies = []
    for piece, kind, offs in zip(pieces, kinds, offsets):
        path, other = kind
        core = 1 - c if other else c
        sign_z = 1 - 2 * lax.rem(z + core, 2)
        sign_x = 1 - 2 * lax.rem(x + core, 2)
        for b, (dz, dx) in enumerate(offs):
            bz = lax.rem(z + dz * sign_z + ZS, ZS)
            bx = lax.rem(x + dx * sign_x + XS, XS)
            row = pl.multiple_of(((bz * XS + bx) * CS + core) * ROWS, ROWS)
            rows = pl.ds(row, ROWS)
            if path == 0:
                copies.append((piece.at[b, :, pl.ds(0, 256)], key.at[rows, :]))
                copies.append((piece.at[b, :, pl.ds(256, 256)], value.at[rows, :]))
                copies.append((piece.at[b, :, pl.ds(512, EXTRA)], query.at[rows, pl.ds(0, EXTRA)]))
            else:
                copies.append((piece.at[b], query.at[rows, pl.ds(EXTRA, 1024 - EXTRA)]))
    started = [pltpu.make_async_copy(s, d, sem.at[i]) for i, (s, d) in enumerate(copies)]
    for copy in started:
        copy.start()
    for copy in started:
        copy.wait()


def placed(pieces):
    kinds = tuple(p[0] for p in pieces)
    offsets = tuple(p[1] for p in pieces)
    count = sum(len(o) * (3 if k[0] == 0 else 1) for k, o in zip(kinds, offsets))
    out = tuple(jax.ShapeDtypeStruct((4096, w), jnp.bfloat16) for w in (1024, 256, 256))
    return pl.pallas_call(
        functools.partial(assemble, kinds, offsets),
        out_shape=out,
        in_specs=[pl.BlockSpec(memory_space=pl.ANY)] * len(pieces),
        out_specs=[pl.BlockSpec(memory_space=pltpu.HBM)] * 3,
        scratch_shapes=[pltpu.SemaphoreType.DMA((count,))],
        compiler_params=pltpu.CompilerParams(vmem_limit_bytes=1 << 20),
        name="assemble",
    )(*[p[2] for p in pieces])


def local(
    w_query,
    first_query,
    second_query,
    w_key,
    first_key,
    second_key,
    w_value,
    first_value,
    second_value,
    norm_train,
    norm_step,
):
    hold_query = hold_rate * first_query + second_query
    whole_query = w_query - learn_rate * hold_query
    hold_key = hold_rate * first_key + second_key
    whole_key = w_key - learn_rate * hold_key
    hold_value = hold_rate * first_value + second_value
    whole_value = w_value - learn_rate * hold_value

    norm = (norm_train + norm_step).astype(jnp.bfloat16).astype(jnp.float32)
    line = jnp.concatenate(
        [
            jnp.sum(jnp.abs(whole_query), axis=0),
            jnp.sum(jnp.abs(whole_key), axis=0),
            jnp.sum(jnp.abs(whole_value), axis=0),
            norm,
            jnp.zeros((112,), jnp.float32),
        ]
    )
    shared = lax.all_to_all(
        jnp.broadcast_to(line[None], (64, 1664)), SHARD, 0, 0, tiled=True
    )
    column = jnp.sum(shared[:, :1536], axis=0) / D_MODEL
    column_query, column_key, column_value = column[:1024], column[1024:1280], column[1280:]
    norms = shared[:, 1536:1552].astype(jnp.bfloat16)

    narrow_query = (whole_query / column_query).astype(jnp.bfloat16)
    narrow_key = (whole_key / column_key).astype(jnp.bfloat16)
    narrow_value = (whole_value / column_value).astype(jnp.bfloat16)

    first = jnp.concatenate([narrow_key, narrow_value, narrow_query[:, :EXTRA]], axis=1)[None]
    second = narrow_query[:, EXTRA:][None]
    cat = functools.partial(jnp.concatenate, axis=0)

    a1 = exchange(first, "x", 0)
    a2 = exchange(cat([first, a1]), "x", 1)
    g = cat([first, a1, a2])
    b1 = exchange(g, "z", 0)
    b2 = exchange(cat([g, b1]), "z", 1)
    b3 = exchange(b2, "z", 0)
    b4 = exchange(b3, "z", 1)
    c1 = exchange(second, "z", 0)
    c2 = exchange(cat([second, c1]), "z", 1)
    c3 = exchange(c2, "z", 0)
    c4 = exchange(c3, "z", 1)
    h = cat([second, c1, c2, c3, c4])
    d1 = exchange(h, "x", 0)
    d2 = exchange(h, "x", 1)
    d3 = exchange(d1, "x", 1)

    xo = (0, 1, -1, -2)
    zo = (0, 1, -1, -2, 2, 3, -3, -4)
    grid = lambda zs, xs: tuple((dz, dx) for dz in zs for dx in xs)
    own = [
        (0, grid((0,), xo), g),
        (0, grid((1,), xo), b1),
        (0, grid((-1, -2), xo), b2),
        (0, grid((2, 3), xo), b3),
        (0, grid((-3, -4), xo), b4),
        (1, grid(zo, (0,)), h),
        (1, grid(zo, (1,)), d1),
        (1, grid(zo, (-1,)), d2),
        (1, grid(zo, (-2,)), d3),
    ]
    pieces = [((p, False), o, a) for p, o, a in own]
    pieces += [((p, True), o, swap_cores(a)) for p, o, a in own]
    serving_query, serving_key, serving_value = placed(pieces)

    n1 = lax.ppermute(norms, "width", [(i, i ^ 1) for i in range(YS)])
    n2 = lax.ppermute(jnp.stack([norms, n1]), "width", [(i, i ^ 3) for i in range(YS)])
    y = lax.axis_index("width")
    near = jnp.stack([norms, n1, n2[1], n2[0]])
    order = jnp.stack([near[j] for j in range(4)])
    pick = [
        jnp.where(y == 0, order[k], jnp.where(y == 1, order[k ^ 1], jnp.where(y == 2, order[k ^ 2], order[k ^ 3])))
        for k in range(4)
    ]
    serve_norm = jnp.stack(pick, axis=1).reshape(4096)
    return (
        serving_query,
        serving_key,
        serving_value,
        column_query,
        column_key,
        column_value,
        serve_norm,
        whole_query,
        whole_key,
        whole_value,
    )


def solution(mesh):
    split = Mesh(
        mesh.devices.reshape(ZS, XS, CS, mesh.shape["width"]),
        SHARD_WIDTH,
    )
    tiles = P(SHARD, "width")
    return jax.shard_map(
        local,
        mesh=split,
        in_specs=(tiles,) * 9 + (P(SHARD_WIDTH),) * 2,
        out_specs=(P(None, "width"),) * 3 + (P("width"),) * 3 + (P(),) + (tiles,) * 3,
        check_vma=False,
    )
```

```python
import functools

import jax
import jax.numpy as jnp
from jax import lax
from jax.experimental import pallas as pl
from jax.experimental.pallas import tpu as pltpu
from jax.sharding import Mesh
from jax.sharding import PartitionSpec as P

D_MODEL = 4096
ZS, XS, CS, YS = 8, 4, 2, 4
SHARD = ("shard_0", "shard_1", "shard_2")
SHARD_WIDTH = ("shard_0", "shard_1", "shard_2", "width")
ROWS = 64
EXTRA = 128

learn_rate = 0.2
hold_rate = 0.8


def exchange(array, dim, phase):
    size = {"z": ZS, "x": XS}[dim]
    pairs = []
    for z in range(ZS):
        for x in range(XS):
            for c in range(CS):
                at = z if dim == "z" else x
                sign = 1 if (at + c) % 2 == 0 else -1
                to = (at + (sign if phase == 0 else -sign)) % size
                tz, tx = (to, x) if dim == "z" else (z, to)
                pairs.append(((z * XS + x) * CS + c, (tz * XS + tx) * CS + c))
    return lax.ppermute(array, SHARD, pairs)


def swap_cores(array):
    return lax.ppermute(array, "shard_2", [(0, 1), (1, 0)])


def assemble(kinds, offsets, aliased, *refs):
    n = len(kinds)
    pieces = refs[:n]
    query, key, value, sem = refs[n + aliased :]
    z, x, c = (lax.axis_index(name) for name in SHARD)
    copies = []
    for piece, kind, offs in zip(pieces, kinds, offsets):
        path, other = kind
        core = 1 - c if other else c
        sign_z = 1 - 2 * lax.rem(z + core, 2)
        sign_x = 1 - 2 * lax.rem(x + core, 2)
        for b, (dz, dx) in enumerate(offs):
            bz = lax.rem(z + dz * sign_z + ZS, ZS)
            bx = lax.rem(x + dx * sign_x + XS, XS)
            row = pl.multiple_of(((bz * XS + bx) * CS + core) * ROWS, ROWS)
            rows = pl.ds(row, ROWS)
            if path == 0:
                copies.append((piece.at[b, :, pl.ds(0, 256)], key.at[rows, :]))
                copies.append((piece.at[b, :, pl.ds(256, 256)], value.at[rows, :]))
                copies.append((piece.at[b, :, pl.ds(512, EXTRA)], query.at[rows, pl.ds(0, EXTRA)]))
            else:
                copies.append((piece.at[b], query.at[rows, pl.ds(EXTRA, 1024 - EXTRA)]))
    started = [pltpu.make_async_copy(s, d, sem.at[i]) for i, (s, d) in enumerate(copies)]
    for copy in started:
        copy.start()
    for copy in started:
        copy.wait()


def placed(pieces, outs, name):
    kinds = tuple(p[0] for p in pieces)
    offsets = tuple(p[1] for p in pieces)
    count = sum(len(o) * (3 if k[0] == 0 else 1) for k, o in zip(kinds, offsets))
    out = tuple(jax.ShapeDtypeStruct((4096, w), jnp.bfloat16) for w in (1024, 256, 256))
    n = len(pieces)
    size = sum(p[2].size for p in pieces) * 2
    return pl.pallas_call(
        functools.partial(assemble, kinds, offsets, len(outs)),
        out_shape=out,
        in_specs=[pl.BlockSpec(memory_space=pl.ANY)] * n
        + [pl.BlockSpec(memory_space=pltpu.HBM)] * len(outs),
        out_specs=[pl.BlockSpec(memory_space=pltpu.HBM)] * 3,
        scratch_shapes=[pltpu.SemaphoreType.DMA((count,))],
        input_output_aliases={n + i: i for i in range(len(outs))},
        compiler_params=pltpu.CompilerParams(vmem_limit_bytes=1 << 20),
        cost_estimate=pl.CostEstimate(flops=5_000_000, bytes_accessed=2 * size, transcendentals=0),
        name=name,
    )(*[p[2] for p in pieces], *outs)


def prepare(*refs):
    inputs, (oq, ok, ov, first, second) = refs[:11], refs[11:16]
    held, sem = refs[16:27], refs[27]
    copies = [pltpu.make_async_copy(i, h, sem.at[n]) for n, (i, h) in enumerate(zip(inputs, held))]
    for copy in copies:
        copy.start()
    for copy in copies:
        copy.wait()
    wq, fq, sq, wk, fk, sk, wv, fv, sv, nt, ns = held
    x, c, y = (lax.axis_index(name) for name in ("shard_1", "shard_2", "width"))
    query = wq[...] - learn_rate * (hold_rate * fq[...] + sq[...])
    key = wk[...] - learn_rate * (hold_rate * fk[...] + sk[...])
    value = wv[...] - learn_rate * (hold_rate * fv[...] + sv[...])
    oq[...], ok[...], ov[...] = query, key, value
    first[0, :ROWS, 0:256] = key
    first[0, :ROWS, 256:512] = value
    first[0, :ROWS, 512:] = query[:, :EXTRA]
    second[0] = query[:, EXTRA:]
    total = lambda a: jnp.sum(jnp.abs(a), axis=0, keepdims=True)
    line = total(query)
    first[0, ROWS:, :] = jnp.zeros((8, 512 + EXTRA), jnp.float32)
    first[0, ROWS : ROWS + 1, 0:512] = line[:, :512]
    first[0, ROWS + 1 : ROWS + 2, 0:512] = line[:, 512:]
    first[0, ROWS + 2 : ROWS + 3, 0:256] = total(key)
    first[0, ROWS + 2 : ROWS + 3, 256:512] = total(value)
    norm = jnp.broadcast_to((nt[...] + ns[...]).astype(jnp.bfloat16), (16, 16))
    lane = lax.broadcasted_iota(jnp.int32, (16, 512), 1)
    spread = (lax.rem(lane, 16) == lax.broadcasted_iota(jnp.int32, (16, 512), 0)).astype(jnp.float32)
    lanes = jnp.dot(norm, spread.astype(jnp.bfloat16), preferred_element_type=jnp.float32)
    slot = (x * CS + c) * YS + y
    lanes = jnp.where(lane // 16 == slot, lanes, 0.0)
    first[0, ROWS + 3 : ROWS + 4, 0:512] = lanes[0:1]


def prepared(*args):
    shape = jax.ShapeDtypeStruct
    f32 = jnp.float32
    return pl.pallas_call(
        prepare,
        out_shape=(
            shape((ROWS, 1024), f32),
            shape((ROWS, 256), f32),
            shape((ROWS, 256), f32),
            shape((1, ROWS + 8, 512 + EXTRA), f32),
            shape((1, ROWS, 1024 - EXTRA), f32),
        ),
        in_specs=[pl.BlockSpec(memory_space=pltpu.HBM)] * 11,
        scratch_shapes=[pltpu.VMEM(a.shape, f32) for a in args] + [pltpu.SemaphoreType.DMA((11,))],
        compiler_params=pltpu.CompilerParams(vmem_limit_bytes=8 << 20),
        cost_estimate=pl.CostEstimate(flops=1_000_000, bytes_accessed=2_000_000, transcendentals=0),
        name="prepare",
    )(*args)


def add_x(p0, p1, p2, out):
    at = slice(ROWS, ROWS + 8)
    line = (p0[0, at, 0:512] + p2[1, at, 0:512]) + (p1[0, at, 0:512] + p2[0, at, 0:512])
    for k in range(4):
        row = line[k : k + 1]
        for j in range(16):
            out[j, :, pl.ds(512 * k, 512)] = row


def added_x(*args):
    return pl.pallas_call(
        add_x,
        out_shape=jax.ShapeDtypeStruct((16, 1, 2048), jnp.float32),
        compiler_params=pltpu.CompilerParams(vmem_limit_bytes=4 << 20),
        cost_estimate=pl.CostEstimate(flops=100_000, bytes_accessed=200_000, transcendentals=0),
        name="add_x",
    )(*args)


def scale(stats, p0, p1, p2, q0, q1, q2, q3, g, h, last, cq, ck, cv, norms):
    line = stats[0]
    for j in range(1, 16):
        line = line + stats[j]
    column = line[:, :1536] / D_MODEL
    query, key, value = column[:, :1024], column[:, 1024:1280], column[:, 1280:]
    cq[...], ck[...], cv[...] = query, key, value
    for z in range(ZS):
        pair = stats[2 * z, :, 1536:] + stats[2 * z + 1, :, 1536:]
        for x in range(XS):
            norms[pl.ds(z * XS + x, 1), :] = pair[:, 128 * x : 128 * x + 128]
    for b, ref in enumerate((q0.at[0], q1.at[0], q2.at[0], q2.at[1], q3.at[0], q3.at[1])):
        block = (ref[...] / query[:, EXTRA:]).astype(jnp.bfloat16)
        h[b] = block
        if b >= 4:
            last[b - 4] = block
    for b, ref in enumerate((p0.at[0], p1.at[0], p2.at[0], p2.at[1])):
        g[b, :, 0:256] = (ref[:ROWS, 0:256] / key).astype(jnp.bfloat16)
        g[b, :, 256:512] = (ref[:ROWS, 256:512] / value).astype(jnp.bfloat16)
        g[b, :, 512:] = (ref[:ROWS, 512:] / query[:, :EXTRA]).astype(jnp.bfloat16)


def scaled(*args):
    shape = jax.ShapeDtypeStruct
    f32, bf16 = jnp.float32, jnp.bfloat16
    return pl.pallas_call(
        scale,
        out_shape=(
            shape((4, ROWS, 512 + EXTRA), bf16),
            shape((6, ROWS, 1024 - EXTRA), bf16),
            shape((2, ROWS, 1024 - EXTRA), bf16),
            shape((1, 1024), f32),
            shape((1, 256), f32),
            shape((1, 256), f32),
            shape((32, 128), f32),
        ),
        compiler_params=pltpu.CompilerParams(vmem_limit_bytes=12 << 20),
        cost_estimate=pl.CostEstimate(flops=2_000_000, bytes_accessed=4_000_000, transcendentals=0),
        name="scale",
    )(*args)


def local(
    w_query,
    first_query,
    second_query,
    w_key,
    first_key,
    second_key,
    w_value,
    first_value,
    second_value,
    norm_train,
    norm_step,
):
    whole_query, whole_key, whole_value, p0, q0 = prepared(
        w_query,
        first_query,
        second_query,
        w_key,
        first_key,
        second_key,
        w_value,
        first_value,
        second_value,
        norm_train.reshape(1, 16),
        norm_step.reshape(1, 16),
    )
    cat = functools.partial(jnp.concatenate, axis=0)
    p1 = exchange(p0, "x", 0)
    q1 = exchange(q0, "z", 0)
    p2 = exchange(cat([p0, p1]), "x", 1)
    q2 = exchange(cat([q0, q1]), "z", 1)
    q3 = exchange(q2, "z", 0)
    stats = lax.all_to_all(added_x(p0, p1, p2), ("shard_0", "shard_2"), 0, 0, tiled=True)
    g, h, last, column_query, column_key, column_value, norms = scaled(
        stats, p0, p1, p2, q0, q1, q2, q3
    )

    b1 = exchange(g, "z", 0)
    b2 = exchange(g, "z", 1)
    b3 = exchange(b1, "z", 1)
    b4 = exchange(b2, "z", 0)
    b5 = exchange(b3, "z", 0)
    b6 = exchange(b4, "z", 1)
    b7 = exchange(b5, "z", 1)
    l0 = exchange(last, "z", 1)
    d1 = exchange(h, "x", 0)
    d2 = exchange(h, "x", 1)
    d3 = exchange(d1, "x", 1)
    l1 = exchange(l0, "x", 0)
    l2 = exchange(l0, "x", 1)
    l3 = exchange(l1, "x", 1)

    xo = (0, 1, -1, -2)
    zh, zl = (0, 1, -1, -2, 2, 3), (-3, -4)
    grid = lambda zs, xs: tuple((dz, dx) for dz in zs for dx in xs)
    own = [
        (0, grid((0,), xo), g),
        (0, grid((1,), xo), b1),
        (0, grid((-1,), xo), b2),
        (0, grid((-2,), xo), b3),
        (0, grid((2,), xo), b4),
        (0, grid((3,), xo), b5),
        (0, grid((-3,), xo), b6),
        (0, grid((-4,), xo), b7),
        (1, grid(zh, (0,)), h),
        (1, grid(zl, (0,)), l0),
        (1, grid(zh, (1,)), d1),
        (1, grid(zh, (-1,)), d2),
        (1, grid(zh, (-2,)), d3),
        (1, grid(zl, (1,)), l1),
        (1, grid(zl, (-1,)), l2),
        (1, grid(zl, (-2,)), l3),
    ]
    stages = (((0, 1, 2, 8, 9), "early"), ((3, 4, 10, 11), "middle"), ((5, 6, 7, 12, 13, 14, 15), "late"))
    outs = ()
    for picks, name in stages:
        pieces = [((own[i][0], False), own[i][1], own[i][2]) for i in picks]
        pieces += [((own[i][0], True), own[i][1], swap_cores(own[i][2])) for i in picks]
        outs = placed(pieces, outs, name)
    serving_query, serving_key, serving_value = outs

    near = [lax.ppermute(norms, "width", [(i, i ^ k) for i in range(YS)]) for k in (1, 2, 3)]
    serve_norm = ((norms + near[0]) + (near[1] + near[2])).astype(jnp.bfloat16).reshape(4096)
    return (
        serving_query,
        serving_key,
        serving_value,
        column_query.reshape(1024),
        column_key.reshape(256),
        column_value.reshape(256),
        serve_norm,
        whole_query,
        whole_key,
        whole_value,
    )


def solution(mesh):
    split = Mesh(
        mesh.devices.reshape(ZS, XS, CS, mesh.shape["width"]),
        SHARD_WIDTH,
    )
    tiles = P(SHARD, "width")
    return jax.shard_map(
        local,
        mesh=split,
        in_specs=(tiles,) * 9 + (P(SHARD_WIDTH),) * 2,
        out_specs=(P(None, "width"),) * 3 + (P("width"),) * 3 + (P(),) + (tiles,) * 3,
        check_vma=False,
    )
```
